8 devices in a mesh: dp: 1 (over z), tp: 8 (over x, y, core).
Axes of the slice: x: 2, y: 2, z: 1, core: 2. Of those that a mesh axis runs over, the one named last changes fastest.
Arguments:
- x: bfloat16 [1792, 5120], P(('dp', 'tp'))
- dy: bfloat16 [1792, 5120], P(('dp', 'tp'))
- pre: bfloat16 [1792, 20480], P('dp', 'tp')
- w_in: bfloat16 [5120, 20480], P(None, 'tp')
- w_down: bfloat16 [20480, 5120], P('tp')
Outputs:
- output 1: bfloat16 [1792, 5120], P(('dp', 'tp'))
- output 2: bfloat16 [5120, 20480], P('dp', 'tp')
- output 3: bfloat16 [20480, 5120], P(('dp', 'tp'))
All inputs are finite; a program needn't handle non-finite values.
Results may differ from the reference program's by a relative error of at most 0.012.
Values are sent between devices in bfloat16 or wider.
A program may use at most 2 GiB of HBM per device.

```python
import jax
import jax.numpy as jnp

ROWS = 1792
D = 5120
FF = 20480


def act(pre):
    return jax.nn.gelu(pre)


def setup_inputs(seed: int = 0, part: int = 0) -> dict:
    kx, ky, ka, ki, kd = jax.random.split(jax.random.key(seed), 5)
    kx, ky, ka = (jax.random.fold_in(k, part) for k in (kx, ky, ka))
    drawn = {
        "x": jax.random.normal(kx, (ROWS, D), jnp.float32),
        "dy": jax.random.normal(ky, (ROWS, D), jnp.float32),
        "pre": jax.random.normal(ka, (ROWS, FF), jnp.float32),
        "w_in": jax.random.normal(ki, (D, FF), jnp.float32) * D**-0.5,
        "w_down": jax.random.normal(kd, (FF, D), jnp.float32) * FF**-0.5,
    }
    return {k: v.astype(jnp.bfloat16) for k, v in drawn.items()}


def reference(x, dy, pre, w_in, w_down):
    hidden, back = jax.vjp(act, pre.astype(jnp.float32))
    d_hidden = jnp.dot(dy, w_down.T, preferred_element_type=jnp.float32)
    d_pre = back(d_hidden)[0].astype(jnp.bfloat16)
    dx = jnp.dot(d_pre, w_in.T, preferred_element_type=jnp.float32)
    dw_in = jnp.dot(x.T, d_pre, preferred_element_type=jnp.float32)
    dw_down = jnp.dot(hidden.astype(jnp.bfloat16).T, dy, preferred_element_type=jnp.float32)
    return tuple(g.astype(jnp.bfloat16) for g in (dx, dw_in, dw_down))
```

```python
import functools

import jax
import jax.numpy as jnp
from jax import lax
from jax.experimental import pallas as pl
from jax.experimental.pallas import tpu as pltpu
from jax.sharding import PartitionSpec as P


BF16, F32 = jnp.bfloat16, jnp.float32
DY_CHUNKS = 4
BLOCK = 512
RING = (0, 1, 3, 2, 6, 7, 5, 4)


def nt(a, b):
    return lax.dot_general(a, b, (((1,), (1,)), ((), ())), preferred_element_type=F32)


def tn(a, b):
    return lax.dot_general(a, b, (((0,), (0,)), ((), ())), preferred_element_type=F32)


def act(pre):
    return jax.nn.gelu(pre)


def cost(flops, nbytes):
    return pl.CostEstimate(flops=int(flops), bytes_accessed=int(nbytes), transcendentals=0)


def once(shape, index):
    return pl.BlockSpec(shape, index, pipeline_mode=pl.Buffered(1))


def chunk_kernel(with_dw, with_acc, first, last, *refs):
    refs = list(refs)
    dy = refs.pop(0)
    if with_dw:
        hidden = refs.pop(0)
    if with_acc:
        w = refs.pop(0)
        acc = None if first else refs.pop(0)
        slope = refs.pop(0) if last else None
    if with_dw:
        if not first:
            refs.pop(0)
        dw = refs.pop(0)
        dw[...] = tn(hidden[...], dy[...]).astype(dw.dtype)
    if with_acc:
        (out,) = refs
        total = nt(dy[...], w[...])
        if not first:
            total = acc[...] + total
        if last:
            total = total * slope[...]
        out[...] = total.astype(out.dtype)


def chunk_call(c, n, dy, hidden, w_down, acc, slope, dw, with_dw=True, with_acc=True):
    first, last = c == 0, c == n - 1
    rows, width = dy.shape
    ff = w_down.shape[0]
    column = pl.BlockSpec((rows, BLOCK), lambda j: (0, j))
    across = pl.BlockSpec((BLOCK, width), lambda j: (j, c))
    ins, specs = [dy], [once((rows, width), lambda j: (0, 0))]
    out_specs, out_shape, aliases = [], [], {}
    flops = nbytes = 0
    if with_dw:
        ins.append(hidden)
        specs.append(column)
    if with_acc:
        ins.append(w_down)
        specs.append(across)
        if not first:
            if not last:
                aliases[len(ins)] = int(with_dw)
            ins.append(acc)
            specs.append(column)
        if last:
            ins.append(slope)
            specs.append(column)
    if with_dw:
        if not first:
            aliases[len(ins)] = 0
            ins.append(dw)
            specs.append(pl.BlockSpec(memory_space=pl.ANY))
        out_specs.append(across)
        out_shape.append(jax.ShapeDtypeStruct(w_down.shape, BF16))
        flops, nbytes = flops + 2 * rows * width * ff, nbytes + 2 * (rows * ff + width * ff)
    if with_acc:
        out_specs.append(column)
        out_shape.append(jax.ShapeDtypeStruct((rows, ff), BF16 if last else F32))
        flops, nbytes = flops + 2 * rows * width * ff, nbytes + 2 * width * ff + 8 * rows * ff
    return pl.pallas_call(
        functools.partial(chunk_kernel, with_dw, with_acc, first, last),
        grid=(ff // BLOCK,),
        in_specs=specs,
        out_specs=out_specs,
        out_shape=out_shape,
        input_output_aliases=aliases,
        cost_estimate=cost(flops, nbytes + 2 * rows * width),
    )(*ins)


def dx_kernel(d_pre, w, out):
    out[...] = nt(d_pre[...], w[...]).astype(out.dtype)


def dx_call(d_pre, w_in, begin, width, block):
    rows, ff = d_pre.shape
    return pl.pallas_call(
        dx_kernel,
        grid=(width // block,),
        in_specs=[once((rows, ff), lambda j: (0, 0)), pl.BlockSpec((block, ff), lambda j: (begin // block + j, 0))],
        out_specs=pl.BlockSpec((rows, block), lambda j: (0, j)),
        out_shape=jax.ShapeDtypeStruct((rows, width), BF16),
        cost_estimate=cost(2 * rows * width * ff, 2 * (rows * ff + width * ff + rows * width)),
    )(d_pre, w_in)


def dw_in_kernel(n, me, starts, d_pre, *refs):
    pieces, (out, x, sem) = refs[:n], refs[n:]
    i, steps = pl.program_id(0), pl.num_programs(0)

    def copies(step, slot):
        columns = pl.ds(pl.multiple_of(step * BLOCK, BLOCK), BLOCK)
        for k, piece in enumerate(pieces):
            at = pl.ds(pl.multiple_of(starts[me[0] * n + k], 16), piece.shape[0])
            yield pltpu.make_async_copy(piece.at[:, columns], x.at[slot, at, :], sem.at[slot])

    @pl.when(i == 0)
    def _():
        for copy in copies(0, 0):
            copy.start()

    @pl.when(i + 1 < steps)
    def _():
        for copy in copies(i + 1, (i + 1) % 2):
            copy.start()

    for copy in copies(i, i % 2):
        copy.wait()
    out[...] = tn(x[i % 2], d_pre[...]).astype(out.dtype)


def dw_in_call(pieces, me, starts, d_pre, width):
    rows, ff = d_pre.shape
    return pl.pallas_call(
        functools.partial(dw_in_kernel, len(pieces)),
        grid_spec=pltpu.PrefetchScalarGridSpec(
            num_scalar_prefetch=2,
            grid=(width // BLOCK,),
            in_specs=[once((rows, ff), lambda i, m, s: (0, 0))] + [pl.BlockSpec(memory_space=pl.ANY)] * len(pieces),
            out_specs=pl.BlockSpec((BLOCK, ff), lambda i, m, s: (i, 0)),
            scratch_shapes=[pltpu.VMEM((2, rows, BLOCK), BF16), pltpu.SemaphoreType.DMA((2,))],
        ),
        out_shape=jax.ShapeDtypeStruct((width, ff), BF16),
        cost_estimate=cost(2 * rows * width * ff, 2 * (rows * ff + width * ff + rows * width)),
        name="dw_in",
    )(me, starts, d_pre, *pieces)


def join_kernel(*refs):
    *parts, out = refs
    begin = 0
    for part in parts:
        out[:, begin : begin + part.shape[1]] = part[...]
        begin += part.shape[1]


def join(parts):
    rows, width = parts[0].shape[0], sum(p.shape[1] for p in parts)
    return pl.pallas_call(
        join_kernel, out_shape=jax.ShapeDtypeStruct((rows, width), BF16), cost_estimate=cost(1, 4 * rows * width), name="join"
    )(*parts)


def solution(mesh):
    tp = mesh.shape["tp"]
    assert tp == len(RING)
    ahead = [(RING[k], RING[(k + 1) % tp]) for k in range(tp)]
    back = [(b, a) for a, b in ahead]
    at = [RING.index(m) for m in range(tp)]

    def step(x, dy, pre, w_in, w_down):
        own, d = x.shape
        half = own // 2
        me = lax.axis_index("tp")
        width = d // DY_CHUNKS
        gathered = [
            lax.all_gather(dy[:, c * width : (c + 1) * width], "tp", axis=0, tiled=True) for c in range(DY_CHUNKS)
        ]
        hidden, back_act = jax.vjp(act, pre.astype(F32))
        slope = back_act(jnp.ones_like(hidden))[0]
        hidden, slope = lax.optimization_barrier((hidden.astype(BF16), slope))

        n, dw, acc = DY_CHUNKS, None, None
        for c in range(n - 1):
            dw, acc = chunk_call(c, n, gathered[c], hidden, w_down, acc, None, dw)
            if c == 0:
                x, acc = lax.optimization_barrier((x, acc))
        pieces = [x]
        starts = [[m * own] for m in range(tp)]
        fore = aft = x
        for k in range(1, tp // 2 + 1):
            whole = k < tp // 2
            if not whole:
                fore, aft = fore[:half], aft[half:]
            fore = lax.ppermute(fore, "tp", ahead)
            aft = lax.ppermute(aft, "tp", back)
            pieces += [fore, aft]
            for m in range(tp):
                starts[m] += [RING[(at[m] - k) % tp] * own, RING[(at[m] + k) % tp] * own + (0 if whole else half)]

        (d_pre,) = chunk_call(n - 1, n, gathered[n - 1], None, w_down, acc, slope, None, with_dw=False)
        dx, begin, ready = [], 0, d_pre
        for cols in (d // 4, d // 4, d // 2):
            part = dx_call(ready, w_in, begin, cols, 256)
            dx.append(lax.psum_scatter(part, "tp", scatter_dimension=0, tiled=True))
            ready, _ = lax.optimization_barrier((ready, part))
            begin += cols
        dw, ready = lax.optimization_barrier((dw, ready))
        (dw,) = chunk_call(n - 1, n, gathered[n - 1], hidden, w_down, None, None, dw, with_acc=False)
        dw, ready = lax.optimization_barrier((dw, ready))
        table = jnp.asarray(sum(starts, []), jnp.int32)
        dw_in = dw_in_call(pieces, me[None].astype(jnp.int32), table, ready, d)
        return join(dx), dw_in, dw

    return jax.shard_map(
        step,
        mesh=mesh,
        in_specs=(P(("dp", "tp"), None), P(("dp", "tp"), None), P("dp", "tp"), P(None, "tp"), P("tp", None)),
        out_specs=(P(("dp", "tp"), None), P("dp", "tp"), P(("dp", "tp"), None)),
        check_vma=False,
    )
```

```python
import functools

import jax
import jax.numpy as jnp
from jax import lax
from jax.experimental import pallas as pl
from jax.experimental.pallas import tpu as pltpu
from jax.sharding import PartitionSpec as P


BF16, F32 = jnp.bfloat16, jnp.float32
CHUNKS = 2
BLOCK = 512
RING = (0, 1, 3, 2, 6, 7, 5, 4)


def nt(a, b):
    return lax.dot_general(a, b, (((1,), (1,)), ((), ())), preferred_element_type=F32)


def tn(a, b):
    return lax.dot_general(a, b, (((0,), (0,)), ((), ())), preferred_element_type=F32)


def act(pre):
    return jax.nn.gelu(pre)


def cost(flops, nbytes):
    return pl.CostEstimate(flops=int(flops), bytes_accessed=int(nbytes), transcendentals=0)


def once(shape, index):
    return pl.BlockSpec(shape, index, pipeline_mode=pl.Buffered(1))


def d_pre_kernel(dy, w, slope, *refs):
    out = refs[-1]
    out[...] = (nt(dy[...], w[...]) * slope[...]).astype(out.dtype)


def d_pre_call(c, dy, w_down, slope, d_pre, block=256):
    rows, d = dy.shape
    ff = w_down.shape[0]
    part = pl.BlockSpec((rows, block), lambda j: (c, j))
    ins = [dy, w_down, slope]
    specs = [once((rows, d), lambda j: (0, 0)), pl.BlockSpec((block, d), lambda j: (j, 0)), part]
    if d_pre is not None:
        ins.append(d_pre)
        specs.append(pl.BlockSpec(memory_space=pl.ANY))
    return pl.pallas_call(
        d_pre_kernel,
        grid=(ff // block,),
        in_specs=specs,
        out_specs=part,
        out_shape=jax.ShapeDtypeStruct(slope.shape, BF16),
        input_output_aliases={} if d_pre is None else {3: 0},
        cost_estimate=cost(2 * rows * d * ff, 2 * (rows * d + d * ff) + 6 * rows * ff),
    )(*ins)


def dx_kernel(d_pre, w, out):
    out[...] = nt(d_pre[...], w[...]).astype(out.dtype)


def dx_call(c, d_pre, w_in, rows, block=512):
    d, ff = w_in.shape
    return pl.pallas_call(
        dx_kernel,
        grid=(d // block,),
        in_specs=[once((rows, ff), lambda j: (c, 0)), pl.BlockSpec((block, ff), lambda j: (j, 0))],
        out_specs=pl.BlockSpec((rows, block), lambda j: (0, j)),
        out_shape=jax.ShapeDtypeStruct((rows, d), BF16),
        cost_estimate=cost(2 * rows * d * ff, 2 * (rows * ff + d * ff + rows * d)),
    )(d_pre, w_in)


def dw_down_kernel(n, hidden, *refs):
    parts, (out, dy, sem) = refs[:n], refs[n:]
    h, i = pl.program_id(0), pl.program_id(1)
    width = dy.shape[2]

    def copies(half, slot):
        columns = pl.ds(pl.multiple_of(half * width, width), width)
        begin = 0
        for part in parts:
            at = pl.ds(begin, part.shape[0])
            yield pltpu.make_async_copy(part.at[:, columns], dy.at[slot, at, :], sem.at[slot])
            begin += part.shape[0]

    @pl.when((h == 0) & (i == 0))
    def _():
        for copy in copies(0, 0):
            copy.start()

    @pl.when((h + 1 < pl.num_programs(0)) & (i == 0))
    def _():
        for copy in copies(h + 1, (h + 1) % 2):
            copy.start()

    @pl.when(i == 0)
    def _():
        for copy in copies(h, h % 2):
            copy.wait()

    out[...] = tn(hidden[...], dy[h % 2]).astype(out.dtype)


def dw_down_call(hidden, parts):
    rows, ff = hidden.shape
    d = parts[0].shape[1]
    width = d // 4
    return pl.pallas_call(
        functools.partial(dw_down_kernel, len(parts)),
        grid=(d // width, ff // BLOCK),
        in_specs=[pl.BlockSpec((rows, BLOCK), lambda h, i: (0, i))] + [pl.BlockSpec(memory_space=pl.ANY)] * len(parts),
        out_specs=pl.BlockSpec((BLOCK, width), lambda h, i: (i, h)),
        out_shape=jax.ShapeDtypeStruct((ff, d), BF16),
        scratch_shapes=[pltpu.VMEM((2, rows, width), BF16), pltpu.SemaphoreType.DMA((2,))],
        cost_estimate=cost(2 * rows * d * ff, 2 * (rows * ff + d * ff + rows * d)),
        name="dw_down",
    )(hidden, *parts)


def dw_in_kernel(n, size, me, starts, d_pre, *refs):
    pieces, (out, x, sem) = refs[:n], refs[n:]
    i, steps = pl.program_id(0), pl.num_programs(0)
    total = x.shape[1] // size

    def copies(step, slot):
        columns = pl.ds(pl.multiple_of(step * BLOCK, BLOCK), BLOCK)
        k = 0
        for piece in pieces:
            for begin in range(0, piece.shape[0], size):
                at = pl.ds(pl.multiple_of(starts[me[0] * total + k], 16), size)
                yield pltpu.make_async_copy(piece.at[pl.ds(begin, size), columns], x.at[slot, at, :], sem.at[slot])
                k += 1

    @pl.when(i == 0)
    def _():
        for copy in copies(0, 0):
            copy.start()

    @pl.when(i + 1 < steps)
    def _():
        for copy in copies(i + 1, (i + 1) % 2):
            copy.start()

    for copy in copies(i, i % 2):
        copy.wait()
    out[...] = tn(x[i % 2], d_pre[...]).astype(out.dtype)


def dw_in_call(pieces, size, me, starts, d_pre, width):
    rows, ff = d_pre.shape
    return pl.pallas_call(
        functools.partial(dw_in_kernel, len(pieces), size),
        grid_spec=pltpu.PrefetchScalarGridSpec(
            num_scalar_prefetch=2,
            grid=(width // BLOCK,),
            in_specs=[once((rows, ff), lambda i, m, s: (0, 0))] + [pl.BlockSpec(memory_space=pl.ANY)] * len(pieces),
            out_specs=pl.BlockSpec((BLOCK, ff), lambda i, m, s: (i, 0)),
            scratch_shapes=[pltpu.VMEM((2, rows, BLOCK), BF16), pltpu.SemaphoreType.DMA((2,))],
        ),
        out_shape=jax.ShapeDtypeStruct((width, ff), BF16),
        cost_estimate=cost(2 * rows * width * ff, 2 * (rows * ff + width * ff + rows * width)),
        name="dw_in",
    )(me, starts, d_pre, *pieces)


def join_kernel(*refs):
    *parts, out = refs
    begin = 0
    for part in parts:
        out[begin : begin + part.shape[0], :] = part[...]
        begin += part.shape[0]


def join(parts):
    rows, width = sum(p.shape[0] for p in parts), parts[0].shape[1]
    return pl.pallas_call(
        join_kernel, out_shape=jax.ShapeDtypeStruct((rows, width), BF16), cost_estimate=cost(1, 4 * rows * width), name="join"
    )(*parts)


def solution(mesh):
    tp = mesh.shape["tp"]
    assert tp == len(RING)
    ahead = [(RING[k], RING[(k + 1) % tp]) for k in range(tp)]
    back = [(b, a) for a, b in ahead]
    at = [RING.index(m) for m in range(tp)]

    def step(x, dy, pre, w_in, w_down):
        own, d = x.shape
        size = own // CHUNKS
        rows = tp * size
        me = lax.axis_index("tp")
        gathered = [
            lax.all_gather(dy[c * size : (c + 1) * size], "tp", axis=0, tiled=True) for c in range(CHUNKS)
        ]
        pre = pre.reshape(tp, CHUNKS, size, -1).swapaxes(0, 1).reshape(pre.shape)
        hidden, back_act = jax.vjp(act, pre.astype(F32))
        slope = back_act(jnp.ones_like(hidden))[0]
        hidden, slope = lax.optimization_barrier((hidden.astype(BF16), slope))

        d_pre, dx = None, []
        for c in range(CHUNKS):
            d_pre = d_pre_call(c, gathered[c], w_down, slope, d_pre)
            if c == 0:
                x, d_pre = lax.optimization_barrier((x, d_pre))
            part = dx_call(c, d_pre, w_in, rows)
            dx.append(lax.psum_scatter(part, "tp", scatter_dimension=0, tiled=True))
            d_pre, _ = lax.optimization_barrier((d_pre, part))

        def begins(m):
            return [c * rows + m * size for c in range(CHUNKS)]

        pieces = [x]
        starts = [begins(m) for m in range(tp)]
        fore = aft = x
        for k in range(1, tp // 2 + 1):
            whole = k < tp // 2
            if not whole:
                fore, aft = fore[:size], aft[size:]
            fore = lax.ppermute(fore, "tp", ahead)
            aft = lax.ppermute(aft, "tp", back)
            pieces += [fore, aft]
            for m in range(tp):
                f, a = begins(RING[(at[m] - k) % tp]), begins(RING[(at[m] + k) % tp])
                starts[m] += f + a if whole else f[:1] + a[1:]

        d_pre, gathered[0] = lax.optimization_barrier((d_pre, gathered[0]))
        dw_down = dw_down_call(hidden, gathered)
        d_pre, dw_down = lax.optimization_barrier((d_pre, dw_down))
        table = jnp.asarray(sum(starts, []), jnp.int32)
        dw_in = dw_in_call(pieces, size, me[None].astype(jnp.int32), table, d_pre, d)
        return join(dx), dw_in, dw_down

    return jax.shard_map(
        step,
        mesh=mesh,
        in_specs=(P(("dp", "tp"), None), P(("dp", "tp"), None), P("dp", "tp"), P(None, "tp"), P("tp", None)),
        out_specs=(P(("dp", "tp"), None), P("dp", "tp"), P(("dp", "tp"), None)),
        check_vma=False,
    )
```
